8 devices in a mesh: batch: 1 (over z), w: 2 (over y), h: 4 (over x, core).
Axes of the slice: x: 2, y: 2, z: 1, core: 2. Of those that a mesh axis runs over, the one named last changes fastest.
Arguments:
- image: bfloat16 [128, 768, 16, 96], P('batch', 'h', 'w')
- down_w1: bfloat16 [3, 3, 96, 192], replicated
- down_v1: float32 [3, 192], replicated
- refine_w1: bfloat16 [3, 3, 192, 192], replicated
- refine_v1: float32 [3, 192], replicated
- down_w2: bfloat16 [3, 3, 192, 384], replicated
- down_v2: float32 [3, 384], replicated
- refine_w2: bfloat16 [3, 3, 384, 384], replicated
- refine_v2: float32 [3, 384], replicated
- down_w3: bfloat16 [3, 3, 384, 768], replicated
- down_v3: float32 [3, 768], replicated
- refine_w3: bfloat16 [3, 3, 768, 768], replicated
- refine_v3: float32 [3, 768], replicated
Outputs:
- output: bfloat16 [128, 96, 2, 768], P('batch', 'h', 'w')
All inputs are finite; a program needn't handle non-finite values.
Results may differ from the reference program's by a relative error of at most 0.00539394.
Values are sent between devices in bfloat16 or wider.
A program may use at most 1 GiB of HBM per device.

```python
import jax
import jax.numpy as jnp
from jax import lax

IMAGES = 128
IMG_HEIGHT = 768
IMG_WIDTH = 16
CHAN_IN = 96
CHAN_ONE = 192
GROUPS = 8
NORM_EPS = 1e-5


def draw_affine(key, channels):
    bias_key, scale_key, shift_key = jax.random.split(key, 3)
    bias = 0.5 * jax.random.normal(bias_key, (channels,), jnp.float32)
    scale = 1.0 + 0.3 * jax.random.normal(scale_key, (channels,), jnp.float32)
    shift = 0.3 * jax.random.normal(shift_key, (channels,), jnp.float32)
    return jnp.stack([bias, scale, shift])


def setup_inputs(seed: int = 0, part: int = 0) -> dict:
    shared_key, image_root = jax.random.split(jax.random.key(seed))
    image_key = jax.random.fold_in(image_root, part)
    noise_key, slope_key, level_key = jax.random.split(image_key, 3)
    noise = jax.random.normal(noise_key, (IMAGES, IMG_HEIGHT, IMG_WIDTH, CHAN_IN), jnp.float32)
    slopes = jax.random.normal(slope_key, (2, IMAGES, 1, 1, CHAN_IN), jnp.float32)
    levels = 0.5 * jax.random.normal(level_key, (IMAGES, 1, 1, CHAN_IN), jnp.float32)
    row_pos = (jnp.arange(IMG_HEIGHT, dtype=jnp.float32) + 0.5) * (2.0 / IMG_HEIGHT) - 1.0
    col_pos = (jnp.arange(IMG_WIDTH, dtype=jnp.float32) + 0.5) * (2.0 / IMG_WIDTH) - 1.0
    ramp = slopes[0] * row_pos[:, None, None] + slopes[1] * col_pos[:, None]
    image = (noise + 1.5 * ramp + levels).astype(jnp.bfloat16)
    widths = [CHAN_IN, CHAN_ONE, 2 * CHAN_ONE, 4 * CHAN_ONE]
    weight_keys = jax.random.split(shared_key, 12)
    inputs = {"image": image}
    for stage in range(3):
        chan_prev = widths[stage]
        chan_next = widths[stage + 1]
        down_w = jax.random.normal(weight_keys[4 * stage], (3, 3, chan_prev, chan_next), jnp.float32) * (9 * chan_prev) ** -0.5
        refine_w = jax.random.normal(weight_keys[4 * stage + 2], (3, 3, chan_next, chan_next), jnp.float32) * (9 * chan_next) ** -0.5
        inputs["down_w" + str(stage + 1)] = down_w.astype(jnp.bfloat16)
        inputs["down_v" + str(stage + 1)] = draw_affine(weight_keys[4 * stage + 1], chan_next)
        inputs["refine_w" + str(stage + 1)] = refine_w.astype(jnp.bfloat16)
        inputs["refine_v" + str(stage + 1)] = draw_affine(weight_keys[4 * stage + 3], chan_next)
    return inputs


def conv_norm(inputs, kernel, affine, stride):
    summed = lax.conv_general_dilated(inputs.astype(jnp.float32), kernel.astype(jnp.float32), (stride, stride), ((1, 1), (1, 1)), dimension_numbers=("NHWC", "HWIO", "NHWC")) + affine[0]
    out_shape = summed.shape
    grouped = summed.reshape(out_shape[0], out_shape[1], out_shape[2], GROUPS, out_shape[3] // GROUPS)
    grp_mean = jnp.mean(grouped, axis=(1, 2, 4), keepdims=True)
    centered = grouped - grp_mean
    grp_var = jnp.mean(jnp.square(centered), axis=(1, 2, 4), keepdims=True)
    normed = (centered * lax.rsqrt(grp_var + NORM_EPS)).reshape(out_shape)
    return jax.nn.relu(normed * affine[1] + affine[2]).astype(jnp.bfloat16)


def reference(image, down_w1, down_v1, refine_w1, refine_v1, down_w2, down_v2, refine_w2, refine_v2, down_w3, down_v3, refine_w3, refine_v3):
    stages = ((down_w1, down_v1, refine_w1, refine_v1), (down_w2, down_v2, refine_w2, refine_v2), (down_w3, down_v3, refine_w3, refine_v3))

    def one_image(single):
        current = single[None]
        for down_w, down_v, refine_w, refine_v in stages:
            current = conv_norm(current, down_w, down_v, 2)
            current = conv_norm(current, refine_w, refine_v, 1)
        return current[0]

    return lax.map(one_image, image)
```

```python
import functools

import jax
import jax.numpy as jnp
from jax import lax
from jax.experimental import pallas as pl
from jax.experimental.pallas import tpu as pltpu
from jax.sharding import PartitionSpec as P

NORM_GROUPS = 8
NORM_EPS = 1e-5
CHUNKS = 2
DIMS = ("HWNC", "HWIO", "HWNC")


def shift_in(piece, axis_name, axis_size):
    if axis_size == 1:
        return jnp.zeros_like(piece)
    return lax.ppermute(piece, axis_name, [(source, source + 1) for source in range(axis_size - 1)])


def total_kernel(row_count, col_count, part_ref, total_ref, got, send_sem, recv_sem):
    row, col = lax.axis_index("h"), lax.axis_index("w")
    count = row_count * col_count
    barrier = pltpu.get_barrier_semaphore()
    peers = []
    for k in range(1, count):
        down, side = k % row_count, k // row_count
        peer_row = row
        for bit in (1, 2, 4, 8):
            if down & bit:
                peer_row = peer_row + bit - 2 * bit * (lax.div(row, bit) % 2)
        peer_col = col
        for bit in (1, 2, 4, 8):
            if side & bit:
                peer_col = peer_col + bit - 2 * bit * (lax.div(col, bit) % 2)
        peers.append({"h": peer_row, "w": peer_col})
    for peer in peers:
        pl.semaphore_signal(barrier, inc=1, device_id=peer, device_id_type=pl.DeviceIdType.MESH)
    pl.semaphore_wait(barrier, count - 1)
    copies = []
    for k, peer in enumerate(peers):
        copy = pltpu.make_async_remote_copy(part_ref, got.at[k], send_sem.at[k], recv_sem.at[k], device_id=peer, device_id_type=pl.DeviceIdType.MESH)
        copy.start()
        copies.append(copy)
    for copy in copies:
        copy.wait()
    terms = [part_ref[...]] + [got[k] for k in range(count - 1)]
    while len(terms) > 1:
        terms = [terms[i] + terms[i + 1] for i in range(0, len(terms), 2)]
    total_ref[...] = terms[0]


def total_sum(part, row_count, col_count):
    count = row_count * col_count
    flat = part.reshape(-1, 128)
    vmem = pl.BlockSpec(memory_space=pltpu.VMEM)
    out = pl.pallas_call(
        functools.partial(total_kernel, row_count, col_count),
        out_shape=jax.ShapeDtypeStruct(flat.shape, jnp.float32),
        in_specs=[vmem],
        out_specs=vmem,
        scratch_shapes=[pltpu.VMEM((count - 1,) + flat.shape, jnp.float32), pltpu.SemaphoreType.DMA((count - 1,)), pltpu.SemaphoreType.DMA((count - 1,))],
        compiler_params=pltpu.CompilerParams(collective_id=0, has_side_effects=True),
        name="total_sum",
    )(flat)
    return out.reshape(part.shape)


def scale_shift(totals, affine, pixel_count):
    per_group = affine.shape[1] // NORM_GROUPS
    count = pixel_count * per_group
    grp_mean = totals[0] / count
    grp_var = jnp.maximum(totals[1] / count - jnp.square(grp_mean), 0.0)
    inv_std = lax.rsqrt(grp_var + NORM_EPS)
    scale = jnp.repeat(inv_std, per_group, axis=1) * affine[1]
    return scale, affine[2] - jnp.repeat(grp_mean * inv_std, per_group, axis=1) * affine[1]


def group_sums(summed):
    both = jnp.stack([jnp.sum(summed, axis=(0, 1)), jnp.sum(jnp.square(summed), axis=(0, 1))])
    return jnp.sum(both.reshape(2, both.shape[1], NORM_GROUPS, -1), axis=3)


def conv_norm(tile, kernel, affine, stride):
    summed = lax.conv_general_dilated(tile, kernel, (stride, stride), ((1, 1), (1, 1)), dimension_numbers=DIMS, preferred_element_type=jnp.float32) + affine[0]
    scale, shift = scale_shift(group_sums(summed), affine, summed.shape[0] * summed.shape[1])
    return jax.nn.relu(summed * scale + shift).astype(jnp.bfloat16)


def pack_kernel(main_ref, edge_ref, scale_ref, shift_ref, out_ref):
    rows, cols, images, chans = main_ref.shape
    dests = out_ref.shape[0]
    part = images // dests
    for dest in range(dests):
        span = pl.ds(dest * part, part)
        scale, shift = scale_ref[span], shift_ref[span]
        done = []
        for col in range(cols):
            value = main_ref[:, col, span]
            if col == 0:
                value = value + edge_ref[:, 0, span]
            done.append(jnp.maximum(value * scale + shift, 0.0))
        for pair in range(0, cols, 2):
            wide = jnp.concatenate([done[pair], done[pair + 1]], axis=-1)
            done[pair] = wide
        both = jnp.concatenate([done[pair] for pair in range(0, cols, 2)], axis=1)
        out_ref[dest] = both.astype(jnp.bfloat16)


def pack(main, edge, scale, shift, chunk, dests):
    rows, cols, images, chans = main.shape
    width = images // CHUNKS
    block = 8
    tall = width // dests * cols // 2
    return pl.pallas_call(
        pack_kernel,
        grid=(rows // block,),
        out_shape=jax.ShapeDtypeStruct((dests, rows, tall, 2 * chans), jnp.bfloat16),
        in_specs=[
            pl.BlockSpec((block, cols, width, chans), lambda i: (i, 0, chunk, 0)),
            pl.BlockSpec((block, 1, width, chans), lambda i: (i, 0, chunk, 0)),
            pl.BlockSpec((width, chans), lambda i: (chunk, 0)),
            pl.BlockSpec((width, chans), lambda i: (chunk, 0)),
        ],
        out_specs=pl.BlockSpec((dests, block, tall, 2 * chans), lambda i: (0, i, 0, 0)),
        compiler_params=pltpu.CompilerParams(vmem_limit_bytes=48 << 20),
        cost_estimate=pl.CostEstimate(flops=40 * rows * cols * width * chans, bytes_accessed=6 * rows * cols * width * chans, transcendentals=0),
        name="pack",
    )(main, edge, scale, shift)


def unpack_kernel(got_ref, out_ref):
    chans = out_ref.shape[2]
    tall = got_ref.shape[3]
    pairs = out_ref.shape[1] // tall // 2
    half = tall // 2
    wide = got_ref.shape[0]
    for side in range(wide):
        value = got_ref[side, 0].astype(jnp.float32)
        pieces = []
        for pair in range(2):
            strip = value[:, pair * half:(pair + 1) * half]
            pieces += [strip[..., :chans], strip[..., chans:]]
        out_ref[:, pl.ds(side * 2 * tall, 2 * tall)] = jnp.concatenate(pieces, axis=1).astype(jnp.bfloat16)


def unpack(got, col_count, row_count):
    _, rows, tall, wide = got.shape
    got = got.reshape(col_count, row_count, rows, tall, wide)
    block = 16
    steps = rows // block
    return pl.pallas_call(
        unpack_kernel,
        grid=(row_count, steps),
        out_shape=jax.ShapeDtypeStruct((row_count * rows, col_count * 2 * tall, wide // 2), jnp.bfloat16),
        in_specs=[pl.BlockSpec((col_count, 1, block, tall, wide), lambda r, i: (0, r, i, 0, 0))],
        out_specs=pl.BlockSpec((block, col_count * 2 * tall, wide // 2), lambda r, i: (r * steps + i, 0, 0)),
        compiler_params=pltpu.CompilerParams(vmem_limit_bytes=48 << 20),
        cost_estimate=pl.CostEstimate(flops=100 * rows * tall * wide * 8, bytes_accessed=4 * rows * tall * wide * 8, transcendentals=0),
        name="unpack",
    )(got)


def solution(mesh):
    row_count = mesh.shape["h"]
    col_count = mesh.shape["w"]
    devices = row_count * col_count
    act_spec = P("batch", "h", "w")

    def first_conv(tile, kernel, affine):
        above = shift_in(tile[:, -1:], "h", row_count)
        left = shift_in(tile[:, :, -1:], "w", col_count)
        left_above = shift_in(above[:, :, -1:], "w", col_count)
        tall = jnp.concatenate([above, tile], axis=1)
        main = lax.conv_general_dilated(tall, kernel, (2, 2), ((0, 0), (1, 0)), dimension_numbers=("NHWC", "HWIO", "HWNC"), preferred_element_type=jnp.float32) + affine[0]
        inner = jnp.arange(main.shape[1]) > 0
        sums = group_sums(main * inner[:, None, None].astype(jnp.float32))
        side = jnp.concatenate([left_above, left], axis=1)
        edge = lax.conv_general_dilated(side, kernel[:, :1], (2, 2), ((0, 0), (0, 0)), dimension_numbers=("NHWC", "HWIO", "HWNC"), preferred_element_type=jnp.float32)
        return main, edge, sums + group_sums(main[:, :1] + edge)

    def local_forward(tile, *params):
        main, edge, sums = first_conv(tile, params[0], params[1])
        rows, cols, images, chans = main.shape
        totals = total_sum(sums, row_count, col_count)
        scale, shift = scale_shift(totals, params[1], rows * cols * devices)
        part = images // (devices * CHUNKS)
        packed = [pack(main, edge, scale, shift, chunk, devices) for chunk in range(CHUNKS)]
        arrived = [lax.all_to_all(piece, ("w", "h"), 0, 0, tiled=True) for piece in packed]
        pieces = []
        for chunk in range(CHUNKS):
            got = arrived[chunk]
            if pieces:
                got, pieces[-1] = lax.optimization_barrier((got, pieces[-1]))
            cur = unpack(got, col_count, row_count)
            cur = cur.reshape(row_count * rows, col_count * cols, part, chans)
            cur = conv_norm(cur, params[2], params[3], 1)
            for stage in (1, 2):
                cur = conv_norm(cur, params[4 * stage], params[4 * stage + 1], 2)
                cur = conv_norm(cur, params[4 * stage + 2], params[4 * stage + 3], 1)
            pieces.append(cur)
        results = []
        for cur in pieces:
            out_rows, out_cols, out_chans = cur.shape[0] // row_count, cur.shape[1] // col_count, cur.shape[3]
            cur = cur.reshape(row_count, out_rows, col_count, out_cols, part, out_chans).transpose(2, 0, 1, 3, 4, 5)
            cur = cur.reshape(devices, out_rows, out_cols, part, out_chans)
            results.append(lax.all_to_all(cur, ("w", "h"), 0, 0, tiled=True))
        whole = jnp.stack(results)
        return whole.transpose(0, 1, 4, 2, 3, 5).reshape(images, *whole.shape[2:4], whole.shape[5])

    return jax.shard_map(local_forward, mesh=mesh, in_specs=(act_spec,) + (P(),) * 12, out_specs=act_spec, check_vma=False)
```

```python
import functools

import jax
import jax.numpy as jnp
from jax import lax
from jax.experimental import pallas as pl
from jax.experimental.pallas import tpu as pltpu
from jax.sharding import PartitionSpec as P


NORM_GROUPS = 8
NORM_EPS = 1e-5
CHUNKS = 2
DIMS = ("HWNC", "HWIO", "HWNC")


def shift_in(piece, axis_name, axis_size):
    if axis_size == 1:
        return jnp.zeros_like(piece)
    return lax.ppermute(piece, axis_name, [(source, source + 1) for source in range(axis_size - 1)])


def total_kernel(row_count, col_count, part_ref, total_ref, got, send_sem, recv_sem):
    row, col = lax.axis_index("h"), lax.axis_index("w")
    count = row_count * col_count
    barrier = pltpu.get_barrier_semaphore()
    peers = []
    for k in range(1, count):
        down, side = k % row_count, k // row_count
        peer_row = row
        for bit in (1, 2, 4, 8):
            if down & bit:
                peer_row = peer_row + bit - 2 * bit * (lax.div(row, bit) % 2)
        peer_col = col
        for bit in (1, 2, 4, 8):
            if side & bit:
                peer_col = peer_col + bit - 2 * bit * (lax.div(col, bit) % 2)
        peers.append({"h": peer_row, "w": peer_col})
    for peer in peers:
        pl.semaphore_signal(barrier, inc=1, device_id=peer, device_id_type=pl.DeviceIdType.MESH)
    pl.semaphore_wait(barrier, count - 1)
    copies = []
    for k, peer in enumerate(peers):
        copy = pltpu.make_async_remote_copy(part_ref, got.at[k], send_sem.at[k], recv_sem.at[k], device_id=peer, device_id_type=pl.DeviceIdType.MESH)
        copy.start()
        copies.append(copy)
    for copy in copies:
        copy.wait()
    terms = [part_ref[...]] + [got[k] for k in range(count - 1)]
    while len(terms) > 1:
        terms = [terms[i] + terms[i + 1] for i in range(0, len(terms), 2)]
    total_ref[...] = terms[0]


def total_sum(part, row_count, col_count):
    count = row_count * col_count
    flat = part.reshape(-1, 128)
    vmem = pl.BlockSpec(memory_space=pltpu.VMEM)
    out = pl.pallas_call(
        functools.partial(total_kernel, row_count, col_count),
        out_shape=jax.ShapeDtypeStruct(flat.shape, jnp.float32),
        in_specs=[vmem],
        out_specs=vmem,
        scratch_shapes=[pltpu.VMEM((count - 1,) + flat.shape, jnp.float32), pltpu.SemaphoreType.DMA((count - 1,)), pltpu.SemaphoreType.DMA((count - 1,))],
        compiler_params=pltpu.CompilerParams(collective_id=0, has_side_effects=True),
        name="total_sum",
    )(flat)
    return out.reshape(part.shape)


def scale_shift(totals, affine, pixel_count):
    per_group = affine.shape[1] // NORM_GROUPS
    count = pixel_count * per_group
    grp_mean = totals[0] / count
    grp_var = jnp.maximum(totals[1] / count - jnp.square(grp_mean), 0.0)
    inv_std = lax.rsqrt(grp_var + NORM_EPS)
    scale = jnp.repeat(inv_std, per_group, axis=1) * affine[1]
    return scale, affine[2] - jnp.repeat(grp_mean * inv_std, per_group, axis=1) * affine[1]


def group_sums(summed):
    both = jnp.stack([jnp.sum(summed, axis=(0, 1)), jnp.sum(jnp.square(summed), axis=(0, 1))])
    return jnp.sum(both.reshape(2, both.shape[1], NORM_GROUPS, -1), axis=3)


def conv_stats(tile, kernel, affine, stride):
    summed = lax.conv_general_dilated(tile, kernel, (stride, stride), ((1, 1), (1, 1)), dimension_numbers=DIMS, preferred_element_type=jnp.float32) + affine[0]
    return (summed, *scale_shift(group_sums(summed), affine, summed.shape[0] * summed.shape[1]))


def conv_norm(tile, kernel, affine, stride):
    summed, scale, shift = conv_stats(tile, kernel, affine, stride)
    return jax.nn.relu(summed * scale + shift).astype(jnp.bfloat16)


def block_scale_shift(sums, squares, affine_ref, pixels):
    chans = sums.shape[1]
    per_group = chans // NORM_GROUPS
    lane = lax.broadcasted_iota(jnp.int32, sums.shape, 1)
    mean, inv = jnp.zeros_like(sums), jnp.zeros_like(sums)
    for group in range(NORM_GROUPS):
        inside = (lane >= group * per_group) & (lane < (group + 1) * per_group)
        grp_mean = jnp.sum(jnp.where(inside, sums, 0.0), axis=1, keepdims=True) / (pixels * per_group)
        grp_square = jnp.sum(jnp.where(inside, squares, 0.0), axis=1, keepdims=True) / (pixels * per_group)
        grp_inv = lax.rsqrt(jnp.maximum(grp_square - jnp.square(grp_mean), 0.0) + NORM_EPS)
        mean = jnp.where(inside, grp_mean, mean)
        inv = jnp.where(inside, grp_inv, inv)
    scale = inv * affine_ref[1:2]
    return scale, affine_ref[2:3] - mean * scale


def last_kernel(part, map_ref, scale_ref, shift_ref, down_hbm, down_v_ref, refine_hbm, refine_v_ref, out_ref, taps, summed, carry, down_w, refine_w, copy_sem):
    step, steps = pl.program_id(0), pl.num_programs(0)
    count, _, cols, _, chans = map_ref.shape
    rows, wide = summed.shape[0] - 2 * part, summed.shape[1]
    out_chans = wide // 2
    down_copy = pltpu.make_async_copy(down_hbm, down_w, copy_sem.at[0])
    refine_copy = pltpu.make_async_copy(refine_hbm, refine_w, copy_sem.at[1])

    @pl.when(step == 0)
    def _():
        down_copy.start()
        refine_copy.start()
        carry[...] = jnp.zeros_like(carry)

    here = pl.ds(pl.multiple_of(step * count * part, count * part), count * part)
    for col in range(cols):
        lanes = slice(col * chans, (col + 1) * chans)
        even = jnp.maximum(map_ref[:, 0, col] * scale_ref[...] + shift_ref[...], 0.0)
        odd = jnp.maximum(map_ref[:, 1, col] * scale_ref[...] + shift_ref[...], 0.0)
        before = jnp.concatenate([carry[:, lanes][None], odd[:-1]], axis=0)
        carry[:, lanes] = odd[count - 1]
        for tap, value in ((0, before), (1, even), (2, odd)):
            taps[tap, here, lanes] = value.reshape(count * part, chans).astype(jnp.bfloat16)

    def convolve(weights, spans, bias_ref):
        block = 256 if rows % 256 == 0 else rows
        sums = [[jnp.zeros((part, out_chans), jnp.float32)] * 2 for _ in spans]

        def body(index, sums):
            start = pl.multiple_of(index * block, block)
            more = []
            for side, (low, high, first) in enumerate(spans):
                value = None
                for tap in range(3):
                    right = weights[tap, first:first + (high - low) // weights.shape[2]].reshape(high - low, out_chans)
                    term = jnp.dot(taps[tap, pl.ds(start, block), low:high], right, preferred_element_type=jnp.float32)
                    value = term if value is None else value + term
                value = value + bias_ref[0:1]
                summed[pl.ds(part + start, block), side * out_chans:(side + 1) * out_chans] = value
                split = value.reshape(block // part, part, out_chans)
                more.append((sums[side][0] + jnp.sum(split, axis=0), sums[side][1] + jnp.sum(split * split, axis=0)))
            return more

        sums = lax.fori_loop(0, rows // block, body, [tuple(pair) for pair in sums])
        return block_scale_shift(sums[0][0] + sums[1][0], sums[0][1] + sums[1][1], bias_ref, rows // part * 2)

    @pl.when(step == steps - 1)
    def _():
        down_copy.wait()
        size = chans
        scale, shift = convolve(down_w, ((0, 2 * size, 1), (size, 4 * size, 0)), down_v_ref)
        block = 128 if rows % 128 == 0 else rows
        for side in range(2):
            lanes = slice(side * out_chans, (side + 1) * out_chans)
            for start in range(0, rows, block):
                for tap in range(3):
                    from_row = start + tap * part
                    value = summed[from_row:from_row + block, lanes].reshape(block // part, part, out_chans)
                    value = jnp.maximum(value * scale + shift, 0.0)
                    zero = jnp.zeros((1, part, out_chans), jnp.float32)
                    if tap == 0 and start == 0:
                        value = jnp.concatenate([zero, value[1:]], axis=0)
                    if tap == 2 and start == rows - block:
                        value = jnp.concatenate([value[:-1], zero], axis=0)
                    taps[tap, start:start + block, lanes] = value.reshape(block, out_chans).astype(jnp.bfloat16)
        refine_copy.wait()
        size = out_chans
        scale, shift = convolve(refine_w, ((0, 2 * size, 1), (0, 2 * size, 0)), refine_v_ref)
        for side in range(2):
            lanes = slice(side * out_chans, (side + 1) * out_chans)
            for start in range(0, rows, block):
                value = summed[part + start:part + start + block, lanes].reshape(block // part, part, out_chans)
                out_ref[side, start:start + block] = jnp.maximum(value * scale + shift, 0.0).reshape(block, out_chans).astype(jnp.bfloat16)


def last_stage(summed, scale, shift, down_w, down_v, refine_w, refine_v):
    rows, cols, part, chans = summed.shape
    out_chans = down_w.shape[3]
    out_rows = rows // 2
    block = 12 if out_rows % 12 == 0 else out_rows
    whole = lambda shape: pl.BlockSpec(shape, lambda i: (0,) * len(shape))
    tall = out_rows * part
    flops = 2 * tall * (5 * 3 * chans * out_chans + 4 * 3 * out_chans * out_chans)
    return pl.pallas_call(
        functools.partial(last_kernel, part),
        grid=(out_rows // block,),
        out_shape=jax.ShapeDtypeStruct((2, tall, out_chans), jnp.bfloat16),
        in_specs=[
            pl.BlockSpec((block, 2, cols, part, chans), lambda i: (i, 0, 0, 0, 0)),
            whole((part, chans)),
            whole((part, chans)),
            pl.BlockSpec(memory_space=pl.ANY),
            whole(down_v.shape),
            pl.BlockSpec(memory_space=pl.ANY),
            whole(refine_v.shape),
        ],
        out_specs=whole((2, tall, out_chans)),
        scratch_shapes=[
            pltpu.VMEM((3, tall, cols * chans), jnp.bfloat16),
            pltpu.VMEM((tall + 2 * part, 2 * out_chans), jnp.float32),
            pltpu.VMEM((part, cols * chans), jnp.float32),
            pltpu.VMEM(down_w.shape, jnp.bfloat16),
            pltpu.VMEM(refine_w.shape, jnp.bfloat16),
            pltpu.SemaphoreType.DMA((2,)),
        ],
        compiler_params=pltpu.CompilerParams(vmem_limit_bytes=56 << 20),
        cost_estimate=pl.CostEstimate(flops=flops, bytes_accessed=4 * rows * cols * part * chans, transcendentals=0),
        name="last_stage",
    )(summed.reshape(out_rows, 2, cols, part, chans), scale, shift, down_w, down_v, refine_w, refine_v)


def edge_kernel(corner_ref, left_ref, kernel_ref, main_ref, col_ref, sum_ref):
    rows, _, images, chans = main_ref.shape
    start = pl.program_id(0) * rows
    total = jnp.zeros((images, chans), jnp.float32)
    square = jnp.zeros((images, chans), jnp.float32)
    for row in range(rows):
        first = 2 * (start + row) - 1
        if row:
            three = left_ref[pl.ds(first, 3)]
        else:
            above = jnp.where(start == 0, corner_ref[...], left_ref[pl.ds(jnp.maximum(first, 0), 1)])
            three = jnp.concatenate([above, left_ref[pl.ds(first + 1, 2)]], axis=0)
        three = three.reshape(three.shape[0] * three.shape[1], images)
        wide = lax.dot_general(three, kernel_ref[...], (((0,), (0,)), ((), ())), preferred_element_type=jnp.float32)
        value = main_ref[row, 0] + wide[:, :chans]
        col_ref[row, 0] = value
        total += value
        square += value * value

    @pl.when(pl.program_id(0) == 0)
    def _():
        sum_ref[...] = jnp.zeros_like(sum_ref)

    sum_ref[0] += total
    sum_ref[1] += square


def edge_column(corner, left, kernel, main):
    rows, _, images, chans = main.shape
    block = 16 if rows % 16 == 0 else 8
    lanes = -(-chans // 128) * 128
    first = jnp.pad(kernel[:, 0], ((0, 0), (0, 0), (0, lanes - chans))).reshape(-1, lanes)
    return pl.pallas_call(
        edge_kernel,
        grid=(rows // block,),
        out_shape=(jax.ShapeDtypeStruct((rows, 1, images, chans), jnp.float32), jax.ShapeDtypeStruct((2, images, chans), jnp.float32)),
        in_specs=[
            pl.BlockSpec(corner.shape, lambda i: (0, 0, 0)),
            pl.BlockSpec(left.shape, lambda i: (0, 0, 0)),
            pl.BlockSpec(first.shape, lambda i: (0, 0)),
            pl.BlockSpec((block, 1, images, chans), lambda i: (i, 0, 0, 0)),
        ],
        out_specs=(pl.BlockSpec((block, 1, images, chans), lambda i: (i, 0, 0, 0)), pl.BlockSpec((2, images, chans), lambda i: (0, 0, 0))),
        compiler_params=pltpu.CompilerParams(vmem_limit_bytes=40 << 20),
        cost_estimate=pl.CostEstimate(flops=2 * rows * images * 288 * chans, bytes_accessed=rows * images * chans * 8, transcendentals=0),
        name="edge_column",
    )(corner, left, first, main)


def pack_kernel(main_ref, first_ref, scale_ref, shift_ref, out_ref):
    _, cols, images, chans = main_ref.shape
    dests = out_ref.shape[0]
    part = images // dests
    for dest in range(dests):
        span = pl.ds(dest * part, part)
        scale, shift = scale_ref[span], shift_ref[span]
        done = []
        for col in range(cols):
            value = main_ref[:, col, span] if col else first_ref[:, 0, span]
            done.append(jnp.maximum(value * scale + shift, 0.0))
        for half in range(2):
            tile = jnp.concatenate(done[half * cols // 2:(half + 1) * cols // 2], axis=1)
            out_ref[dest, :, :, half * chans:(half + 1) * chans] = tile.astype(jnp.bfloat16)


def pack(main, first, scale, shift, chunk, dests):
    rows, cols, images, chans = main.shape
    width = images // CHUNKS
    block = 8
    tall = width // dests * cols // 2
    return pl.pallas_call(
        pack_kernel,
        grid=(rows // block,),
        out_shape=jax.ShapeDtypeStruct((dests, rows, tall, 2 * chans), jnp.bfloat16),
        in_specs=[
            pl.BlockSpec((block, cols, width, chans), lambda i: (i, 0, chunk, 0)),
            pl.BlockSpec((block, 1, width, chans), lambda i: (i, 0, chunk, 0)),
            pl.BlockSpec((width, chans), lambda i: (chunk, 0)),
            pl.BlockSpec((width, chans), lambda i: (chunk, 0)),
        ],
        out_specs=pl.BlockSpec((dests, block, tall, 2 * chans), lambda i: (0, i, 0, 0)),
        compiler_params=pltpu.CompilerParams(vmem_limit_bytes=48 << 20),
        cost_estimate=pl.CostEstimate(flops=40 * rows * cols * width * chans, bytes_accessed=6 * rows * cols * width * chans, transcendentals=0),
        name="pack",
    )(main, first, scale, shift)


def unpack_kernel(got_ref, out_ref):
    chans = out_ref.shape[2]
    tall = got_ref.shape[3]
    for side in range(got_ref.shape[0]):
        for half in range(2):
            first = (2 * side + half) * tall
            out_ref[:, first:first + tall] = got_ref[side, 0, :, :, half * chans:(half + 1) * chans]


def unpack(got, col_count, row_count):
    _, rows, tall, wide = got.shape
    got = got.reshape(col_count, row_count, rows, tall, wide)
    block = rows // 2
    steps = 2
    return pl.pallas_call(
        unpack_kernel,
        grid=(row_count, steps),
        out_shape=jax.ShapeDtypeStruct((row_count * rows, col_count * 2 * tall, wide // 2), jnp.bfloat16),
        in_specs=[pl.BlockSpec((col_count, 1, block, tall, wide), lambda r, i: (0, r, i, 0, 0))],
        out_specs=pl.BlockSpec((block, col_count * 2 * tall, wide // 2), lambda r, i: (r * steps + i, 0, 0)),
        compiler_params=pltpu.CompilerParams(vmem_limit_bytes=48 << 20),
        cost_estimate=pl.CostEstimate(flops=100 * rows * tall * wide * 8, bytes_accessed=4 * rows * tall * wide * 8, transcendentals=0),
        name="unpack",
    )(got)


def solution(mesh):
    row_count = mesh.shape["h"]
    col_count = mesh.shape["w"]
    devices = row_count * col_count
    act_spec = P("batch", "h", "w")

    def left_column(tile):
        column = tile[:, :, -1].transpose(1, 2, 0)
        if col_count == 1:
            return jnp.zeros_like(column[:1]), jnp.zeros_like(column)
        pairs = [(col * row_count + row - 1, (col + 1) * row_count + row) for col in range(col_count - 1) for row in range(1, row_count)]
        corner = lax.ppermute(column[-1:], ("w", "h"), pairs)
        return corner, lax.ppermute(column, "w", [(col, col + 1) for col in range(col_count - 1)])

    def main_conv(tile, kernel, affine):
        tall = jnp.concatenate([shift_in(tile[:, -1:], "h", row_count), tile], axis=1)
        main = lax.conv_general_dilated(tall, kernel, (2, 2), ((0, 0), (1, 0)), dimension_numbers=("NHWC", "HWIO", "HWNC"), preferred_element_type=jnp.float32) + affine[0]
        inner = jnp.arange(main.shape[1]) > 0
        return main, group_sums(main * inner[:, None, None].astype(jnp.float32))

    def local_forward(tile, *params):
        corner, left = left_column(tile)
        main, sums = main_conv(tile, params[0], params[1])
        rows, cols, images, chans = main.shape
        part = images // (devices * CHUNKS)
        first, more = edge_column(corner, left, params[0], main)
        totals = total_sum(sums + jnp.sum(more.reshape(2, images, NORM_GROUPS, -1), axis=3), row_count, col_count)
        scale, shift = scale_shift(totals, params[1], rows * cols * devices)
        arrived = []
        for chunk in range(CHUNKS):
            packed = pack(main, first, scale, shift, chunk, devices)
            arrived.append(lax.all_to_all(packed, ("w", "h"), 0, 0, tiled=True))
        results = []
        for chunk in range(CHUNKS):
            got = arrived[chunk]
            if chunk:
                got, _ = lax.optimization_barrier((got, cur))
            cur = unpack(got, col_count, row_count)
            cur = cur.reshape(row_count * rows, col_count * cols, part, chans)
            cur = conv_norm(cur, params[2], params[3], 1)
            cur = conv_norm(cur, params[4], params[5], 2)
            cur = last_stage(*conv_stats(cur, params[6], params[7], 1), *params[8:12])
            out_rows, out_chans = cur.shape[1] // (row_count * part), cur.shape[2]
            home = cur.reshape(devices, out_rows, 1, part, out_chans)
            results.append(lax.all_to_all(home, ("w", "h"), 0, 0, tiled=True))
        whole = jnp.stack(results)
        return whole.transpose(0, 1, 4, 2, 3, 5).reshape(images, *whole.shape[2:4], whole.shape[5])

    return jax.shard_map(local_forward, mesh=mesh, in_specs=(act_spec,) + (P(),) * 12, out_specs=act_spec, check_vma=False)
```

```python
import functools

import jax
import jax.numpy as jnp
from jax import lax
from jax.experimental import pallas as pl
from jax.experimental.pallas import tpu as pltpu
from jax.sharding import PartitionSpec as P


NORM_GROUPS = 8
NORM_EPS = 1e-5
CHUNKS = 2
BANDS = 2
PARTS = (2, 1)
DIMS = ("HWNC", "HWIO", "HWNC")


def shift_in(piece, axis_name, axis_size):
    if axis_size == 1:
        return jnp.zeros_like(piece)
    return lax.ppermute(piece, axis_name, [(source, source + 1) for source in range(axis_size - 1)])


def total_kernel(row_count, col_count, part_ref, total_ref, got, send_sem, recv_sem):
    row, col = lax.axis_index("h"), lax.axis_index("w")
    count = row_count * col_count
    barrier = pltpu.get_barrier_semaphore()
    peers = []
    for k in range(1, count):
        down, side = k % row_count, k // row_count
        peer_row = row
        for bit in (1, 2, 4, 8):
            if down & bit:
                peer_row = peer_row + bit - 2 * bit * (lax.div(row, bit) % 2)
        peer_col = col
        for bit in (1, 2, 4, 8):
            if side & bit:
                peer_col = peer_col + bit - 2 * bit * (lax.div(col, bit) % 2)
        peers.append({"h": peer_row, "w": peer_col})
    for peer in peers:
        pl.semaphore_signal(barrier, inc=1, device_id=peer, device_id_type=pl.DeviceIdType.MESH)
    pl.semaphore_wait(barrier, count - 1)
    copies = []
    for k, peer in enumerate(peers):
        copy = pltpu.make_async_remote_copy(part_ref, got.at[k], send_sem.at[k], recv_sem.at[k], device_id=peer, device_id_type=pl.DeviceIdType.MESH)
        copy.start()
        copies.append(copy)
    for copy in copies:
        copy.wait()
    terms = [part_ref[...]] + [got[k] for k in range(count - 1)]
    while len(terms) > 1:
        terms = [terms[i] + terms[i + 1] for i in range(0, len(terms), 2)]
    total_ref[...] = terms[0]


def total_sum(part, row_count, col_count):
    count = row_count * col_count
    flat = part.reshape(-1, 128)
    vmem = pl.BlockSpec(memory_space=pltpu.VMEM)
    out = pl.pallas_call(
        functools.partial(total_kernel, row_count, col_count),
        out_shape=jax.ShapeDtypeStruct(flat.shape, jnp.float32),
        in_specs=[vmem],
        out_specs=vmem,
        scratch_shapes=[pltpu.VMEM((count - 1,) + flat.shape, jnp.float32), pltpu.SemaphoreType.DMA((count - 1,)), pltpu.SemaphoreType.DMA((count - 1,))],
        compiler_params=pltpu.CompilerParams(collective_id=0, has_side_effects=True),
        name="total_sum",
    )(flat)
    return out.reshape(part.shape)


def scale_shift(totals, affine, pixel_count):
    per_group = affine.shape[1] // NORM_GROUPS
    count = pixel_count * per_group
    grp_mean = totals[0] / count
    grp_var = jnp.maximum(totals[1] / count - jnp.square(grp_mean), 0.0)
    inv_std = lax.rsqrt(grp_var + NORM_EPS)
    scale = jnp.repeat(inv_std, per_group, axis=1) * affine[1]
    return scale, affine[2] - jnp.repeat(grp_mean * inv_std, per_group, axis=1) * affine[1]


def group_sums(summed):
    both = jnp.stack([jnp.sum(summed, axis=(0, 1)), jnp.sum(jnp.square(summed), axis=(0, 1))])
    return jnp.sum(both.reshape(2, both.shape[1], NORM_GROUPS, -1), axis=3)


def conv_stats(tile, kernel, affine, stride):
    summed = lax.conv_general_dilated(tile, kernel, (stride, stride), ((1, 1), (1, 1)), dimension_numbers=DIMS, preferred_element_type=jnp.float32) + affine[0]
    return (summed, *scale_shift(group_sums(summed), affine, summed.shape[0] * summed.shape[1]))


def conv_norm(tile, kernel, affine, stride):
    summed, scale, shift = conv_stats(tile, kernel, affine, stride)
    return jax.nn.relu(summed * scale + shift).astype(jnp.bfloat16)


def block_scale_shift(sums, squares, affine_ref, pixels):
    chans = sums.shape[1]
    per_group = chans // NORM_GROUPS
    lane = lax.broadcasted_iota(jnp.int32, sums.shape, 1)
    mean, inv = jnp.zeros_like(sums), jnp.zeros_like(sums)
    for group in range(NORM_GROUPS):
        inside = (lane >= group * per_group) & (lane < (group + 1) * per_group)
        grp_mean = jnp.sum(jnp.where(inside, sums, 0.0), axis=1, keepdims=True) / (pixels * per_group)
        grp_square = jnp.sum(jnp.where(inside, squares, 0.0), axis=1, keepdims=True) / (pixels * per_group)
        grp_inv = lax.rsqrt(jnp.maximum(grp_square - jnp.square(grp_mean), 0.0) + NORM_EPS)
        mean = jnp.where(inside, grp_mean, mean)
        inv = jnp.where(inside, grp_inv, inv)
    scale = inv * affine_ref[1:2]
    return scale, affine_ref[2:3] - mean * scale


def last_kernel(part, map_ref, scale_ref, shift_ref, down_hbm, down_v_ref, refine_hbm, refine_v_ref, out_ref, taps, summed, carry, down_w, refine_w, copy_sem):
    step, steps = pl.program_id(0), pl.num_programs(0)
    count, _, cols, _, chans = map_ref.shape
    rows, wide = summed.shape[0] - 2 * part, summed.shape[1]
    out_chans = wide // 2
    down_copy = pltpu.make_async_copy(down_hbm, down_w, copy_sem.at[0])
    refine_copy = pltpu.make_async_copy(refine_hbm, refine_w, copy_sem.at[1])

    @pl.when(step == 0)
    def _():
        down_copy.start()
        refine_copy.start()
        carry[...] = jnp.zeros_like(carry)

    here = pl.ds(pl.multiple_of(step * count * part, count * part), count * part)
    for col in range(cols):
        lanes = slice(col * chans, (col + 1) * chans)
        even = jnp.maximum(map_ref[:, 0, col] * scale_ref[...] + shift_ref[...], 0.0)
        odd = jnp.maximum(map_ref[:, 1, col] * scale_ref[...] + shift_ref[...], 0.0)
        before = jnp.concatenate([carry[:, lanes][None], odd[:-1]], axis=0)
        carry[:, lanes] = odd[count - 1]
        for tap, value in ((0, before), (1, even), (2, odd)):
            taps[tap, here, lanes] = value.reshape(count * part, chans).astype(jnp.bfloat16)

    def convolve(weights, spans, bias_ref, places):
        block = rows
        sums = [[jnp.zeros((part, out_chans), jnp.float32)] * 2 for _ in spans]

        def body(index, sums):
            start = pl.multiple_of(index * block, block)
            more = []
            for side, (low, high, first) in enumerate(spans):
                value = None
                for tap in range(3):
                    right = weights[tap, first:first + (high - low) // weights.shape[2]].reshape(high - low, out_chans)
                    term = jnp.dot(taps[places[tap][0], pl.ds(start + places[tap][1], block), low:high], right, preferred_element_type=jnp.float32)
                    value = term if value is None else value + term
                value = value + bias_ref[0:1]
                summed[pl.ds(part + start, block), side * out_chans:(side + 1) * out_chans] = value
                split = value.reshape(block // part, part, out_chans)
                more.append((sums[side][0] + jnp.sum(split, axis=0), sums[side][1] + jnp.sum(split * split, axis=0)))
            return more

        sums = lax.fori_loop(0, rows // block, body, [tuple(pair) for pair in sums])
        return block_scale_shift(sums[0][0] + sums[1][0], sums[0][1] + sums[1][1], bias_ref, rows // part * 2)

    @pl.when(step == steps - 1)
    def _():
        down_copy.wait()
        size = chans
        scale, shift = convolve(down_w, ((0, 2 * size, 1), (size, 4 * size, 0)), down_v_ref, ((0, 0), (1, 0), (2, 0)))
        block = 128 if rows % 128 == 0 else rows
        zero = jnp.zeros((1, part, out_chans), jnp.float32)
        for side in range(2):
            lanes = slice(side * out_chans, (side + 1) * out_chans)
            for start in range(0, rows + block, block):
                size = block + part if start < rows else 2 * part
                value = summed[start:start + size, lanes].reshape(size // part, part, out_chans)
                value = jnp.maximum(value * scale + shift, 0.0)
                if start == 0:
                    value = jnp.concatenate([zero, value[1:]], axis=0)
                if start < rows:
                    taps[1, start:start + block, lanes] = value[1:].reshape(block, out_chans).astype(jnp.bfloat16)
                    value = value[:-1]
                else:
                    value = jnp.concatenate([value[:1], zero], axis=0)
                taps[0, start:start + value.shape[0] * part, lanes] = value.reshape(-1, out_chans).astype(jnp.bfloat16)
        refine_copy.wait()
        size = out_chans
        scale, shift = convolve(refine_w, ((0, 2 * size, 1), (0, 2 * size, 0)), refine_v_ref, ((0, 0), (1, 0), (0, 2 * part)))
        block = rows * 2 // out_ref.shape[0]
        for side in range(2):
            lanes = slice(side * out_chans, (side + 1) * out_chans)
            for place, start in enumerate(range(0, rows, block)):
                value = summed[part + start:part + start + block, lanes].reshape(block // part, part, out_chans)
                value = jnp.maximum(value * scale + shift, 0.0)
                out_ref[side * (rows // block) + place] = jnp.swapaxes(value, 0, 1).astype(jnp.bfloat16)


def last_stage(row_count, summed, scale, shift, down_w, down_v, refine_w, refine_v):
    rows, cols, part, chans = summed.shape
    out_chans = down_w.shape[3]
    out_rows = rows // 2
    block = out_rows // 2 if out_rows % 2 == 0 else out_rows
    whole = lambda shape: pl.BlockSpec(shape, lambda i: (0,) * len(shape))
    tall = out_rows * part
    flops = 2 * tall * (5 * 3 * chans * out_chans + 4 * 3 * out_chans * out_chans)
    return pl.pallas_call(
        functools.partial(last_kernel, part),
        grid=(out_rows // block,),
        out_shape=jax.ShapeDtypeStruct((2 * row_count, part, out_rows // row_count, out_chans), jnp.bfloat16),
        in_specs=[
            pl.BlockSpec((block, 2, cols, part, chans), lambda i: (i, 0, 0, 0, 0)),
            whole((part, chans)),
            whole((part, chans)),
            pl.BlockSpec(memory_space=pl.ANY),
            whole(down_v.shape),
            pl.BlockSpec(memory_space=pl.ANY),
            whole(refine_v.shape),
        ],
        out_specs=whole((2 * row_count, part, out_rows // row_count, out_chans)),
        scratch_shapes=[
            pltpu.VMEM((3, tall + 2 * part, cols * chans), jnp.bfloat16),
            pltpu.VMEM((tall + 2 * part, 2 * out_chans), jnp.float32),
            pltpu.VMEM((part, cols * chans), jnp.float32),
            pltpu.VMEM(down_w.shape, jnp.bfloat16),
            pltpu.VMEM(refine_w.shape, jnp.bfloat16),
            pltpu.SemaphoreType.DMA((2,)),
        ],
        compiler_params=pltpu.CompilerParams(vmem_limit_bytes=56 << 20),
        cost_estimate=pl.CostEstimate(flops=flops, bytes_accessed=4 * rows * cols * part * chans, transcendentals=0),
        name="last_stage",
    )(summed.reshape(out_rows, 2, cols, part, chans), scale, shift, down_w, down_v, refine_w, refine_v)


def edge_kernel(corner_ref, left_ref, kernel_ref, main_ref, *refs):
    col_ref, sum_ref = refs[-2:]
    rows, _, images, chans = main_ref.shape
    start = pl.program_id(0) * rows
    total = jnp.zeros((images, chans), jnp.float32)
    square = jnp.zeros((images, chans), jnp.float32)
    for row in range(rows):
        first = 2 * (start + row) - 1
        if row:
            three = left_ref[pl.ds(first, 3)]
        else:
            above = jnp.where(start == 0, corner_ref[...], left_ref[pl.ds(jnp.maximum(first, 0), 1)])
            three = jnp.concatenate([above, left_ref[pl.ds(first + 1, 2)]], axis=0)
        three = three.reshape(three.shape[0] * three.shape[1], images)
        wide = lax.dot_general(three, kernel_ref[...], (((0,), (0,)), ((), ())), preferred_element_type=jnp.float32)
        value = main_ref[row, 0] + wide[:, :chans]
        col_ref[row, 0] = value
        total += value
        square += value * value

    @pl.when(pl.program_id(0) == 0)
    def _():
        sum_ref[...] = jnp.zeros_like(sum_ref)

    sum_ref[0] += total
    sum_ref[1] += square


def edge_column(corner, left, kernel, main, whole, band):
    height, _, images, chans = main.shape
    rows = height // BANDS
    ahead = band * rows
    block = 16 if rows % 16 == 0 else 8
    ahead = ahead // block
    lanes = -(-chans // 128) * 128
    first = jnp.pad(kernel[:, 0], ((0, 0), (0, 0), (0, lanes - chans))).reshape(-1, lanes)
    return pl.pallas_call(
        edge_kernel,
        grid=(rows // block,),
        out_shape=(jax.ShapeDtypeStruct((height, 1, images, chans), jnp.float32), jax.ShapeDtypeStruct((2, images, chans), jnp.float32)),
        in_specs=[
            pl.BlockSpec(corner.shape, lambda i: (0, 0, 0)),
            pl.BlockSpec(left.shape, lambda i: (0, 0, 0)),
            pl.BlockSpec(first.shape, lambda i: (0, 0)),
            pl.BlockSpec((block, 1, images, chans), lambda i: (ahead + i, 0, 0, 0)),
        ] + [pl.BlockSpec(memory_space=pl.ANY)] * (whole is not None),
        input_output_aliases={} if whole is None else {4: 0},
        out_specs=(pl.BlockSpec((block, 1, images, chans), lambda i: (ahead + i, 0, 0, 0)), pl.BlockSpec((2, images, chans), lambda i: (0, 0, 0))),
        compiler_params=pltpu.CompilerParams(vmem_limit_bytes=40 << 20),
        cost_estimate=pl.CostEstimate(flops=2 * rows * images * 288 * chans, bytes_accessed=rows * images * chans * 8, transcendentals=0),
        name="edge_column",
    )(*((corner, left, first, main) if whole is None else (corner, left, first, main, whole)))


def pack_kernel(main_ref, first_ref, scale_ref, shift_ref, out_ref):
    _, cols, images, chans = main_ref.shape
    dests = out_ref.shape[0]
    part = images // dests
    for dest in range(dests):
        span = pl.ds(dest * part, part)
        scale, shift = scale_ref[span], shift_ref[span]
        done = []
        for col in range(cols):
            value = main_ref[:, col, span] if col else first_ref[:, 0, span]
            done.append(jnp.maximum(value * scale + shift, 0.0))
        for half in range(2):
            tile = jnp.concatenate(done[half * cols // 2:(half + 1) * cols // 2], axis=1)
            out_ref[dest, :, :, half * chans:(half + 1) * chans] = tile.astype(jnp.bfloat16)


def pack(main, first, scale, shift, chunk, band, dests):
    rows, cols, images, chans = main.shape
    rows = rows // PARTS[chunk]
    width = images // CHUNKS
    block = 8
    tall = width // dests * cols // 2
    ahead = band * rows // block
    return pl.pallas_call(
        pack_kernel,
        grid=(rows // block,),
        out_shape=jax.ShapeDtypeStruct((dests, rows, tall, 2 * chans), jnp.bfloat16),
        in_specs=[
            pl.BlockSpec((block, cols, width, chans), lambda i: (ahead + i, 0, chunk, 0)),
            pl.BlockSpec((block, 1, width, chans), lambda i: (ahead + i, 0, chunk, 0)),
            pl.BlockSpec((width, chans), lambda i: (chunk, 0)),
            pl.BlockSpec((width, chans), lambda i: (chunk, 0)),
        ],
        out_specs=pl.BlockSpec((dests, block, tall, 2 * chans), lambda i: (0, i, 0, 0)),
        compiler_params=pltpu.CompilerParams(vmem_limit_bytes=48 << 20),
        cost_estimate=pl.CostEstimate(flops=40 * rows * cols * width * chans, bytes_accessed=6 * rows * cols * width * chans, transcendentals=0),
        name="pack",
    )(main, first, scale, shift)


def unpack_kernel(got_ref, *refs):
    out_ref = refs[-1]
    chans = out_ref.shape[2]
    tall = got_ref.shape[3]
    for side in range(got_ref.shape[0]):
        for half in range(2):
            first = (2 * side + half) * tall
            out_ref[:, first:first + tall] = got_ref[side, 0, :, :, half * chans:(half + 1) * chans]


def unpack(got, whole, band, bands, col_count, row_count):
    _, rows, tall, wide = got.shape
    got = got.reshape(col_count, row_count, rows, tall, wide)
    shape = (row_count * rows * bands, col_count * 2 * tall, wide // 2)
    return pl.pallas_call(
        unpack_kernel,
        grid=(row_count,),
        out_shape=jax.ShapeDtypeStruct(shape, jnp.bfloat16),
        in_specs=[pl.BlockSpec((col_count, 1, rows, tall, wide), lambda r: (0, r, 0, 0, 0))] + [pl.BlockSpec(memory_space=pl.ANY)] * (whole is not None),
        out_specs=pl.BlockSpec((rows,) + shape[1:], lambda r: (r * bands + band, 0, 0)),
        input_output_aliases={} if whole is None else {1: 0},
        compiler_params=pltpu.CompilerParams(vmem_limit_bytes=48 << 20),
        cost_estimate=pl.CostEstimate(flops=100 * rows * tall * wide * 8, bytes_accessed=4 * rows * tall * wide * 8, transcendentals=0),
        name="unpack",
    )(*((got,) if whole is None else (got, whole)))


def gather_kernel(got_ref, *refs):
    refs[-1][...] = got_ref[...]


def gather(got, whole, chunk):
    images, rows, chans = got.shape
    steps = 4
    block = (images // steps, rows, chans)
    return pl.pallas_call(
        gather_kernel,
        grid=(steps,),
        out_shape=jax.ShapeDtypeStruct((images * CHUNKS, rows, chans), got.dtype),
        in_specs=[pl.BlockSpec(block, lambda i: (i, 0, 0))] + [pl.BlockSpec(memory_space=pl.ANY)] * (whole is not None),
        out_specs=pl.BlockSpec(block, lambda i: (chunk * steps + i, 0, 0)),
        input_output_aliases={} if whole is None else {1: 0},
        name="gather",
    )(*((got,) if whole is None else (got, whole)))


def solution(mesh):
    row_count = mesh.shape["h"]
    col_count = mesh.shape["w"]
    devices = row_count * col_count
    act_spec = P("batch", "h", "w")

    def left_column(tile):
        column = tile[:, :, -1].transpose(1, 2, 0)
        size = column.shape[0] // BANDS
        if col_count == 1:
            return [(jnp.zeros_like(column[:1]), jnp.zeros_like(column[:size]))] * BANDS
        pairs = [(col * row_count + row - 1, (col + 1) * row_count + row) for col in range(col_count - 1) for row in range(1, row_count)]
        above = lax.ppermute(column[-1:], ("w", "h"), pairs)
        got = []
        for band in range(BANDS):
            piece = lax.ppermute(column[band * size:(band + 1) * size], "w", [(col, col + 1) for col in range(col_count - 1)])
            got.append((above, piece))
            above = piece[-1:]
        return got

    def main_conv(tile, kernel, affine):
        above = shift_in(tile[:, -1:], "h", row_count)
        tall = jnp.concatenate([above, tile], axis=1)
        main = lax.conv_general_dilated(tall, kernel, (2, 2), ((0, 0), (1, 0)), dimension_numbers=("NHWC", "HWIO", "HWNC"), preferred_element_type=jnp.float32) + affine[0]
        inner = jnp.arange(main.shape[1]) > 0
        return main, group_sums(main * inner[:, None, None].astype(jnp.float32))

    def local_forward(tile, *params):
        lefts = left_column(tile)
        main, sums = main_conv(tile, params[0], params[1])
        rows, cols, images, chans = main.shape
        part = images // (devices * CHUNKS)
        first = None
        for band in range(BANDS):
            corner, left = lefts[band]
            first, more = edge_column(corner, left, params[0], main, first, band)
            sums = sums + jnp.sum(more.reshape(2, images, NORM_GROUPS, -1), axis=3)
        totals = total_sum(sums, row_count, col_count)
        scale, shift = scale_shift(totals, params[1], rows * cols * devices)
        arrived = []
        for chunk in range(CHUNKS):
            arrived.append([])
            for band in range(PARTS[chunk]):
                packed = pack(main, first, scale, shift, chunk, band, devices)
                arrived[chunk].append(lax.all_to_all(packed, ("w", "h"), 0, 0, tiled=True))
        results = []
        for chunk in range(CHUNKS):
            whole = None
            for band, got in enumerate(arrived[chunk]):
                if chunk:
                    got, _ = lax.optimization_barrier((got, cur))
                whole = unpack(got, whole, band, PARTS[chunk], col_count, row_count)
            cur = whole
            cur = cur.reshape(row_count * rows, col_count * cols, part, chans)
            cur = conv_norm(cur, params[2], params[3], 1)
            cur = conv_norm(cur, params[4], params[5], 2)
            cur = last_stage(row_count, *conv_stats(cur, params[6], params[7], 1), *params[8:12])
            results.append(lax.all_to_all(cur, ("w", "h"), 0, 0, tiled=True))
        whole = None
        for chunk, result in enumerate(results):
            whole = gather(result.reshape(-1, *result.shape[2:]), whole, chunk)
        return whole[:, :, None]

    return jax.shard_map(local_forward, mesh=mesh, in_specs=(act_spec,) + (P(),) * 12, out_specs=act_spec, check_vma=False)
```
